32 devices in a mesh: ep: 8 (over z, x), tp: 4 (over y, core).
Axes of the slice: x: 2, y: 2, z: 4, core: 2. Of those that a mesh axis runs over, the one named last changes fastest.
Arguments:
- tokens: bfloat16 [1024, 4096], P('ep', 'tp'), may hold values from -6 to 6
- expert_ids: int32 [1024, 2], P('ep'), may hold values from 0 to 7, all different within a row; in each aligned block of 128 rows (0 to 127, 128 to 255, ...) at most 40 rows name the same one
- gates: float32 [1024, 2], P('ep'), may hold values from 0.1 to 1
- gate_weight: bfloat16 [4096, 57344], P('tp', 'ep'), may hold values from -0.09375 to 0.09375
- up_weight: bfloat16 [4096, 57344], P('tp', 'ep'), may hold values from -0.09375 to 0.09375
- down_weight: bfloat16 [57344, 4096], P('ep', 'tp'), may hold values from -0.0625 to 0.0625
Outputs:
- mixed: bfloat16 [1024, 4096], P('ep', 'tp')
- expert_counts: float32 [8], replicated
- aux_loss: float32 [], replicated
The draws below stay inside these ranges and needn't reach their ends.
Inputs may be any that keep to these rules, and one draw needn't show every extreme that they name: `expert_ids`: each token names 2 different experts. Among the tokens of one index of ep no expert is named more than 40 times, and in every draw some expert is named exactly 40 times by some index's tokens; every expert is named somewhere.
All inputs are finite; a program needn't handle non-finite values.
Results may differ from the reference program's by a relative error of at most 0.008.
Values may be sent and summed in bfloat16 or wider, within the bound.
A program may use at most 128 MiB of HBM per device.

```python
import math
import jax
import jax.numpy as jnp
import numpy as np
from jax import lax

D = 4096
FF = 7168
EXPERTS = 8
TOP = 2
TOK_DEV = 128
CAP = 40
REPLICAS = 1
TOKENS = 1024
N_EP = 8


def block_scale(stream_key, dims, shards, smallest, high):
    def one(axis_at, parts):
        steps = jax.random.uniform(jax.random.fold_in(jax.random.fold_in(stream_key, 6), axis_at), (parts,), jnp.float32, smallest / len(shards), high / len(shards))
        return jnp.repeat(jnp.exp(steps), dims[axis_at] // parts).reshape((-1,) + (1,) * (len(dims) - axis_at - 1))

    level = one(*shards[0])
    for cut in shards[1:]:
        level = level * one(*cut)
    return level


def routed_block(stream_key, own, number, rows, count, top, bound, lean):
    ranking = jax.random.permutation(stream_key, count)
    crowded, ordinary = load_shares(count, rows * top, bound, lean, True), load_shares(count, rows * top, bound, lean, False)
    places = jnp.arange(count)

    def named(lengths, offset_by):
        used = int((lengths > 0).sum())
        fixed = max(1, used // 4)
        moved = fixed + (places - fixed + offset_by * (used - fixed)) % max(1, count - fixed)
        return jnp.zeros((count,), jnp.int32).at[ranking[jnp.where(places < fixed, places, moved)]].set(jnp.asarray(lengths, jnp.int32))

    lengths = jnp.where(number % 4 == 0, named(crowded, number // 4), named(ordinary, number - number // 4 - 1))
    mixed = jax.random.permutation(jax.random.fold_in(own, 3), count)
    source_of, taker = mixed[0:count // 2 * 2:2], mixed[1:count // 2 * 2:2]
    room = jnp.minimum(lengths[source_of] - 1, bound - lengths[taker]) // 2
    room = jnp.where((source_of == ranking[0]) | (taker == ranking[0]) | (lengths[taker] == 0), 0, jnp.maximum(room, 0))
    moved = jax.random.randint(jax.random.fold_in(own, 4), (count // 2,), 0, 1 << 20) % (room + 1)
    lengths = lengths.at[source_of].add(-moved).at[taker].add(moved)
    members = jnp.searchsorted(jnp.cumsum(lengths), jnp.arange(rows * top), side="right").astype(jnp.int32)
    table = members.reshape(top, rows).T
    table = table[jax.random.permutation(jax.random.fold_in(own, 1), rows)]
    offset_by = jax.random.randint(jax.random.fold_in(own, 2), (rows, 1), 0, top)
    return jnp.take_along_axis(table, (jnp.arange(top)[None, :] + offset_by) % top, axis=1)


def load_shares(count, total, limit, slope, full):
    loads = [(1 << 20) // math.isqrt(standing ** slope) + 1 for standing in range(1, count + 1)]
    largest = limit if full else min(limit, max(-(-total // count), total * loads[0] // sum(loads)))
    least = 1 if total - largest >= count - 1 else 0
    given, spare = [largest] + [least] * (count - 1), total - largest - least * (count - 1)
    while spare > 0:
        candidates = [i for i in range(1, count) if given[i] < largest] or [i for i in range(1, count) if given[i] < limit]
        pool, left = sum([loads[i] for i in candidates]), spare
        for i in candidates:
            extra = min(limit - given[i], max(1, left * loads[i] // pool), spare)
            given[i] = given[i] + extra
            spare = spare - extra
    return np.array(given)


def normal_values(stream_key, extent, scale, limit, cuts=(), held_as=jnp.bfloat16):
    array = jax.random.normal(stream_key, extent, jnp.float32) * scale
    if len(cuts) > 0:
        array = block_scale(stream_key, extent, cuts, -0.22, 0.18) * array
    return jnp.clip(array, min=-limit, max=limit).astype(held_as)


def setup_inputs(seed: int = 0) -> dict:
    key_of = jax.random.split(jax.random.key(seed), 7)
    tokens = normal_values(key_of[0], (TOKENS, D), 1.0, 6.0, ((0, 8), (1, 4)))
    expert_ids_keys = jax.random.split(jax.random.fold_in(key_of[1], 1), TOKENS // TOK_DEV)
    expert_ids_turns = jax.random.permutation(jax.random.fold_in(key_of[1], 3), TOKENS // TOK_DEV)
    expert_ids = jax.vmap(lambda own, number: routed_block(jax.random.fold_in(key_of[1], 2), own, number, TOK_DEV, EXPERTS, TOP, CAP, 2))(expert_ids_keys, expert_ids_turns).reshape((TOKENS, TOP))
    gates = jnp.clip(0.1 + 0.9 * jax.random.uniform(key_of[2], (TOKENS, TOP), jnp.float32) ** block_scale(key_of[2], (TOKENS, TOP), ((0, 8),), -0.2, 0.2), 0.1, 1.0)
    gate_weight = normal_values(key_of[3], (D, EXPERTS * FF), D ** -0.5, 0.09375, ((0, 4), (1, 8)))
    up_weight = normal_values(key_of[4], (D, EXPERTS * FF), D ** -0.5, 0.09375, ((0, 4), (1, 8)))
    down_weight = normal_values(key_of[5], (EXPERTS * FF, D), FF ** -0.5, 0.0625, ((0, 8), (1, 4)))
    return dict(tokens=tokens, expert_ids=expert_ids, gates=gates, gate_weight=gate_weight, up_weight=up_weight, down_weight=down_weight)


def reference(tokens, expert_ids, gates, gate_weight, up_weight, down_weight):
    assign = TOK_DEV * TOP
    ids = expert_ids.reshape(N_EP, assign)
    onehot = (ids[:, :, None] == jnp.arange(EXPERTS, dtype=jnp.int32)[None, None, :]).astype(jnp.int32)
    before = jnp.cumsum(onehot, axis=1) - onehot
    slot = jnp.sum(before * onehot, axis=2)
    target = ids * CAP + slot
    place = (target[:, :, None] == jnp.arange(EXPERTS * CAP, dtype=jnp.int32)[None, None, :]).astype(jnp.float32)
    blocks = jnp.repeat(tokens.reshape(N_EP, TOK_DEV, D), TOP, axis=1).astype(jnp.float32)
    dispatched = jnp.einsum("jas,jad->jsd", place, blocks, precision=lax.Precision.HIGHEST).astype(jnp.bfloat16)
    per_expert = dispatched.reshape(N_EP, EXPERTS, CAP, D).transpose(1, 0, 2, 3).reshape(EXPERTS, N_EP * CAP, D)
    gate_cols = gate_weight.reshape(D, EXPERTS, FF).transpose(1, 0, 2)
    up_cols = up_weight.reshape(D, EXPERTS, FF).transpose(1, 0, 2)
    down_rows = down_weight.reshape(EXPERTS, FF, D)

    def expert(operands):
        rows, gate_e, up_e, down_e = operands
        gate = jnp.dot(rows, gate_e, preferred_element_type=jnp.float32)
        upper = jnp.dot(rows, up_e, preferred_element_type=jnp.float32)
        hidden = (jax.nn.silu(gate) * upper).astype(jnp.bfloat16)
        pieces = hidden.reshape(-1, REPLICAS, FF // REPLICAS).astype(jnp.float32)
        downs = down_e.reshape(REPLICAS, FF // REPLICAS, D).astype(jnp.float32)
        partial_value = jnp.einsum("nrf,rfd->rnd", pieces, downs).astype(jnp.bfloat16)
        partial_value = lax.optimization_barrier(partial_value)
        return jnp.sum(partial_value.astype(jnp.float32), axis=0)

    outputs = lax.map(expert, (per_expert, gate_cols, up_cols, down_rows))
    results = outputs.reshape(EXPERTS, N_EP, CAP, D).transpose(1, 0, 2, 3).reshape(N_EP, EXPERTS * CAP, D)
    weighted = place * gates.reshape(N_EP, assign)[:, :, None]
    combine = weighted.reshape(N_EP, TOK_DEV, TOP, EXPERTS * CAP).sum(axis=2)
    mixed = jnp.einsum("jts,jsd->jtd", combine, results, precision=lax.Precision.HIGHEST)
    mixed = mixed.reshape(TOKENS, D).astype(jnp.bfloat16)
    counts = jnp.sum(onehot, axis=(0, 1)).astype(jnp.float32)
    totals = jnp.sum(onehot.astype(jnp.float32) * gates.reshape(N_EP, assign)[:, :, None], axis=(0, 1))
    aux_loss = EXPERTS * jnp.sum(counts / (TOP * TOKENS) * (totals / TOKENS))
    return mixed, counts, aux_loss
```

```python
import functools

import jax
import jax.numpy as jnp
from jax import lax
from jax.experimental import pallas as pl
from jax.experimental.pallas import tpu as pltpu
from jax.sharding import PartitionSpec as P

EXPERTS = 8
TOP = 2
CAP = 40
MESH = pl.DeviceIdType.MESH
RECV = 8
LOCAL = 4
WEIGHTS = 3


def for_pieces(count, body):
    piece = max(p for p in range(16, 321, 16) if count % p == 0)
    if piece == count:
        body(0, piece)
        return

    def step(i, carry):
        body(pl.multiple_of(i * piece, piece), piece)
        return carry

    lax.fori_loop(0, count // piece, step, 0)


def expert_kernel(
    steps, chunk, x_ref, gate_hbm, up_hbm, down_hbm, out_ref,
    gate_w, up_w, down_w, near_send, near_recv, keep, far_send, far_recv, own, hidden, total,
    weight_sem, near_s, near_r, far_s, far_r, share_s, share_r, give_s, give_r, pass_s, pass_r,
):
    rows = x_ref.shape[0]
    half = rows // 2
    quarter = rows // 4
    me = lax.axis_index("tp")
    low = lax.rem(me, 2)
    high = me // 2
    near = high * 2 + (1 - low)
    far = (1 - high) * 2 + low
    keep_at = pl.multiple_of(low * half, half)
    send_at = pl.multiple_of((1 - low) * half, half)
    mine_in = pl.multiple_of(high * quarter, quarter)
    other_in = pl.multiple_of((1 - high) * quarter, quarter)
    mine = pl.multiple_of(low * half + high * quarter, quarter)
    other = pl.multiple_of(low * half + (1 - high) * quarter, quarter)

    barrier = pltpu.get_barrier_semaphore()
    for peer in (near, far):
        pl.semaphore_signal(barrier, inc=1, device_id={"tp": peer}, device_id_type=MESH)

    def remote(src, dst, send, recv, peer):
        return pltpu.make_async_remote_copy(
            src_ref=src, dst_ref=dst, send_sem=send, recv_sem=recv,
            device_id={"tp": peer}, device_id_type=MESH,
        )

    def columns(i):
        return pl.ds(pl.multiple_of(i * chunk, chunk), chunk)

    def load_gate(i):
        s = lax.rem(i, WEIGHTS)
        return pltpu.make_async_copy(gate_hbm.at[:, columns(i)], gate_w.at[s], weight_sem.at[0, s])

    def load_up(i):
        s = lax.rem(i, WEIGHTS)
        return pltpu.make_async_copy(up_hbm.at[:, columns(i)], up_w.at[s], weight_sem.at[1, s])

    def load_down(i):
        s = lax.rem(i, WEIGHTS)
        return pltpu.make_async_copy(down_hbm.at[columns(i), :], down_w.at[s], weight_sem.at[2, s])

    def near_copy(i):
        s, r = lax.rem(i, LOCAL), lax.rem(i, RECV)
        return remote(near_send.at[s], near_recv.at[r], near_s.at[s], near_r.at[r], near)

    def far_copy(i):
        s, r = lax.rem(i, LOCAL), lax.rem(i, RECV)
        return remote(far_send.at[s], far_recv.at[r], far_s.at[s], far_r.at[r], far)

    def block(i, at):
        return hidden.at[lax.rem(i, RECV), pl.ds(at, quarter), :]

    def share_copy(i):
        r = lax.rem(i, RECV)
        return remote(block(i, mine), block(i, mine), share_s.at[r], share_r.at[r], far)

    def give_copy(i):
        r = lax.rem(i, RECV)
        return remote(block(i, mine), block(i, mine), give_s.at[r], give_r.at[r], near)

    def pass_copy(i):
        r = lax.rem(i, RECV)
        return remote(block(i, other), block(i, other), pass_s.at[r], pass_r.at[r], near)

    for i in range(min(2, steps)):
        load_gate(i).start()
        load_up(i).start()

    def clear(at, size):
        total[pl.ds(at, size), :] = jnp.zeros((size, total.shape[1]), jnp.float32)

    for_pieces(rows, clear)
    pl.semaphore_wait(barrier, 2)

    def iteration(i, carry):
        @pl.when(i + 2 < steps)
        def _():
            load_gate(i + 2).start()
            load_up(i + 2).start()

        @pl.when((i >= 4) & (i - 4 < steps))
        def _():
            load_down(i - 4).start()

        @pl.when(i < steps)
        def _():
            load_gate(i).wait()
            load_up(i).wait()
            s = lax.rem(i, LOCAL)
            w = lax.rem(i, WEIGHTS)

            def sent(at, size):
                x = x_ref[pl.ds(send_at + at, size), :]
                for k, weight in enumerate((gate_w, up_w)):
                    near_send[s, pl.ds(at, size), k * chunk:(k + 1) * chunk] = jnp.dot(
                        x, weight[w], preferred_element_type=jnp.float32
                    ).astype(jnp.bfloat16)

            for_pieces(half, sent)
            near_copy(i).start()

            def kept(at, size):
                x = x_ref[pl.ds(keep_at + at, size), :]
                for k, weight in enumerate((gate_w, up_w)):
                    keep[s, pl.ds(at, size), k * chunk:(k + 1) * chunk] = jnp.dot(
                        x, weight[w], preferred_element_type=jnp.float32
                    )

            for_pieces(half, kept)

        @pl.when((i >= 1) & (i - 1 < steps))
        def _():
            j = i - 1
            s, r = lax.rem(j, LOCAL), lax.rem(j, RECV)
            near_copy(j).wait()

            def summed(at, size):
                far_send[s, pl.ds(at, size), :] = (
                    keep[s, pl.ds(other_in + at, size), :]
                    + near_recv[r, pl.ds(other_in + at, size), :].astype(jnp.float32)
                ).astype(jnp.bfloat16)

            for_pieces(quarter, summed)
            far_copy(j).start()

            def held(at, size):
                own[s, pl.ds(at, size), :] = (
                    keep[s, pl.ds(mine_in + at, size), :]
                    + near_recv[r, pl.ds(mine_in + at, size), :].astype(jnp.float32)
                )

            for_pieces(quarter, held)

        @pl.when((i >= 3) & (i - 3 < steps))
        def _():
            j = i - 3
            s, r = lax.rem(j, LOCAL), lax.rem(j, RECV)
            far_copy(j).wait()

            def activate(at, size):
                both = own[s, pl.ds(at, size), :] + far_recv[r, pl.ds(at, size), :].astype(jnp.float32)
                gate_pre = both[:, :chunk]
                up_pre = both[:, chunk:]
                hidden[r, pl.ds(mine + at, size), :] = (
                    gate_pre / (1.0 + jnp.exp(-gate_pre)) * up_pre
                ).astype(jnp.bfloat16)

            for_pieces(quarter, activate)
            share_copy(j).start()
            give_copy(j).start()

        @pl.when((i >= 5) & (i - 5 < steps))
        def _():
            share_copy(i - 5).wait()
            pass_copy(i - 5).start()

        @pl.when((i >= 6) & (i - 6 < steps))
        def _():
            j = i - 6
            r, w = lax.rem(j, RECV), lax.rem(j, WEIGHTS)
            give_copy(j).wait()
            pass_copy(j).wait()
            load_down(j).wait()

            def add(at, size):
                total[pl.ds(at, size), :] += jnp.dot(
                    hidden[r, pl.ds(at, size), :], down_w[w], preferred_element_type=jnp.float32
                )

            for_pieces(rows, add)

        return carry

    lax.fori_loop(0, steps + 6, iteration, 0)

    def finish(at, size):
        out_ref[pl.ds(at, size), :] = total[pl.ds(at, size), :].astype(jnp.bfloat16)

    for_pieces(rows, finish)


def expert_rows(received, gate_weight, up_weight, down_weight):
    rows, depth = received.shape
    width = gate_weight.shape[1]
    out = down_weight.shape[1]
    chunk = 256 if width % 256 == 0 else 128
    steps = width // chunk
    half, quarter = rows // 2, rows // 4
    vmem, hbm = pl.BlockSpec(memory_space=pltpu.VMEM), pl.BlockSpec(memory_space=pl.ANY)
    dma = pltpu.SemaphoreType.DMA
    bf16, f32 = jnp.bfloat16, jnp.float32
    return pl.pallas_call(
        functools.partial(expert_kernel, steps, chunk),
        out_shape=jax.ShapeDtypeStruct((rows, out), bf16),
        in_specs=[vmem, hbm, hbm, hbm],
        out_specs=vmem,
        scratch_shapes=[
            pltpu.VMEM((WEIGHTS, depth, chunk), bf16),
            pltpu.VMEM((WEIGHTS, depth, chunk), bf16),
            pltpu.VMEM((WEIGHTS, chunk, out), bf16),
            pltpu.VMEM((LOCAL, half, 2 * chunk), bf16),
            pltpu.VMEM((RECV, half, 2 * chunk), bf16),
            pltpu.VMEM((LOCAL, half, 2 * chunk), f32),
            pltpu.VMEM((LOCAL, quarter, 2 * chunk), bf16),
            pltpu.VMEM((RECV, quarter, 2 * chunk), bf16),
            pltpu.VMEM((LOCAL, quarter, 2 * chunk), f32),
            pltpu.VMEM((RECV, rows, chunk), bf16),
            pltpu.VMEM((rows, out), f32),
            dma((3, WEIGHTS)),
            dma((LOCAL,)), dma((RECV,)),
            dma((LOCAL,)), dma((RECV,)),
            dma((RECV,)), dma((RECV,)),
            dma((RECV,)), dma((RECV,)),
            dma((RECV,)), dma((RECV,)),
        ],
        compiler_params=pltpu.CompilerParams(
            collective_id=0, has_side_effects=True, vmem_limit_bytes=60 * 1024 * 1024
        ),
        cost_estimate=pl.CostEstimate(
            flops=2 * rows * width * (2 * depth + out),
            bytes_accessed=2 * width * (2 * depth + out),
            transcendentals=0,
        ),
    )(received, gate_weight, up_weight, down_weight)


def per_device(tokens, expert_ids, gates, gate_weight, up_weight, down_weight):
    count_tok = tokens.shape[0]
    quarter = tokens.shape[1]
    replicas = lax.axis_size("ep") // EXPERTS
    slots_all = EXPERTS * CAP
    flat_ids = expert_ids.reshape(-1)
    onehot = (flat_ids[:, None] == jnp.arange(EXPERTS, dtype=jnp.int32)[None, :]).astype(jnp.int32)
    before = jnp.cumsum(onehot, axis=0) - onehot
    target = flat_ids * CAP + jnp.sum(before * onehot, axis=1)
    matches = (
        target.reshape(count_tok, TOP)[:, :, None]
        == jnp.arange(slots_all, dtype=jnp.int32)[None, None, :]
    ).astype(jnp.float32)
    combine = jnp.sum(matches * gates[:, :, None], axis=1)
    selector = jnp.sum(matches, axis=1).astype(jnp.bfloat16)
    dispatched = jnp.einsum(
        "ts,td->sd", selector, tokens, preferred_element_type=jnp.float32
    ).astype(jnp.bfloat16)
    copies = jnp.broadcast_to(
        dispatched.reshape(EXPERTS, 1, CAP, quarter), (EXPERTS, replicas, CAP, quarter)
    )
    received = lax.all_to_all(
        copies.reshape(-1, quarter), "ep", split_axis=0, concat_axis=0, tiled=True
    )
    partial_value = expert_rows(received, gate_weight, up_weight, down_weight)
    returned = lax.all_to_all(partial_value, "ep", split_axis=0, concat_axis=0, tiled=True)
    results = jnp.sum(returned.reshape(EXPERTS, replicas, CAP, quarter).astype(jnp.float32), axis=1)
    results = results.reshape(slots_all, quarter)
    mixed = jnp.dot(
        combine, results, precision=lax.Precision.HIGHEST, preferred_element_type=jnp.float32
    ).astype(jnp.bfloat16)
    counts = jnp.sum(onehot, axis=0).astype(jnp.float32)
    totals = jnp.sum(onehot.astype(jnp.float32) * gates.reshape(-1)[:, None], axis=0)
    counts, totals = lax.psum((counts, totals), "ep")
    tokens_all = count_tok * lax.axis_size("ep")
    aux_loss = EXPERTS * jnp.sum(counts / (TOP * tokens_all) * (totals / tokens_all))
    return (mixed, counts, aux_loss)


def solution(mesh):
    placed = (
        P("ep", "tp"),
        P("ep", None),
        P("ep", None),
        P("tp", "ep"),
        P("tp", "ep"),
        P("ep", "tp"),
    )
    return jax.shard_map(
        per_device, mesh=mesh, in_specs=placed, out_specs=(P("ep", "tp"), P(), P()), check_vma=False
    )
```

```python
import functools

import jax
import jax.numpy as jnp
from jax import lax
from jax.experimental import pallas as pl
from jax.experimental.pallas import tpu as pltpu
from jax.sharding import PartitionSpec as P

EXPERTS = 8
TOP = 2
CAP = 40
MESH = pl.DeviceIdType.MESH
RECV = 8
LOCAL = 4
WEIGHTS = 3


def for_pieces(count, body):
    piece = max(p for p in range(16, 321, 16) if count % p == 0)
    if piece == count:
        body(0, piece)
        return

    def step(i, carry):
        body(pl.multiple_of(i * piece, piece), piece)
        return carry

    lax.fori_loop(0, count // piece, step, 0)


def expert_kernel(
    steps, chunk, x_ref, gate_hbm, up_hbm, down_hbm, out_ref,
    gate_w, up_w, down_w, near_send, near_recv, keep, far_send, far_recv, own, hidden, total,
    weight_sem, near_s, near_r, far_s, far_r, share_s, share_r, give_s, give_r, pass_s, pass_r,
):
    rows = x_ref.shape[0]
    half = rows // 2
    quarter = rows // 4
    me = lax.axis_index("tp")
    low = lax.rem(me, 2)
    high = me // 2
    near = high * 2 + (1 - low)
    far = (1 - high) * 2 + low
    keep_at = pl.multiple_of(low * half, half)
    send_at = pl.multiple_of((1 - low) * half, half)
    mine_in = pl.multiple_of(high * quarter, quarter)
    other_in = pl.multiple_of((1 - high) * quarter, quarter)
    mine = pl.multiple_of(low * half + high * quarter, quarter)
    other = pl.multiple_of(low * half + (1 - high) * quarter, quarter)

    barrier = pltpu.get_barrier_semaphore()
    for peer in (near, far):
        pl.semaphore_signal(barrier, inc=1, device_id={"tp": peer}, device_id_type=MESH)

    def remote(src, dst, send, recv, peer):
        return pltpu.make_async_remote_copy(
            src_ref=src, dst_ref=dst, send_sem=send, recv_sem=recv,
            device_id={"tp": peer}, device_id_type=MESH,
        )

    def columns(i):
        return pl.ds(pl.multiple_of(i * chunk, chunk), chunk)

    def load_gate(i):
        s = lax.rem(i, WEIGHTS)
        return pltpu.make_async_copy(gate_hbm.at[:, columns(i)], gate_w.at[s], weight_sem.at[0, s])

    def load_up(i):
        s = lax.rem(i, WEIGHTS)
        return pltpu.make_async_copy(up_hbm.at[:, columns(i)], up_w.at[s], weight_sem.at[1, s])

    def load_down(i):
        s = lax.rem(i, WEIGHTS)
        return pltpu.make_async_copy(down_hbm.at[columns(i), :], down_w.at[s], weight_sem.at[2, s])

    def near_copy(i):
        s, r = lax.rem(i, LOCAL), lax.rem(i, RECV)
        return remote(near_send.at[s], near_recv.at[r], near_s.at[s], near_r.at[r], near)

    def far_copy(i):
        s, r = lax.rem(i, LOCAL), lax.rem(i, RECV)
        return remote(far_send.at[s], far_recv.at[r], far_s.at[s], far_r.at[r], far)

    def block(i, at):
        return hidden.at[lax.rem(i, RECV), pl.ds(at, quarter), :]

    def share_copy(i):
        r = lax.rem(i, RECV)
        return remote(block(i, mine), block(i, mine), share_s.at[r], share_r.at[r], far)

    def give_copy(i):
        r = lax.rem(i, RECV)
        return remote(block(i, mine), block(i, mine), give_s.at[r], give_r.at[r], near)

    def pass_copy(i):
        r = lax.rem(i, RECV)
        return remote(block(i, other), block(i, other), pass_s.at[r], pass_r.at[r], near)

    for i in range(min(2, steps)):
        load_gate(i).start()
        load_up(i).start()

    def clear(at, size):
        total[pl.ds(at, size), :] = jnp.zeros((size, total.shape[1]), jnp.float32)

    for_pieces(rows, clear)
    pl.semaphore_wait(barrier, 2)

    def iteration(i, carry):
        @pl.when(i + 2 < steps)
        def _():
            load_gate(i + 2).start()
            load_up(i + 2).start()

        @pl.when((i >= 4) & (i - 4 < steps))
        def _():
            load_down(i - 4).start()

        @pl.when(i < steps)
        def _():
            load_gate(i).wait()
            load_up(i).wait()
            s = lax.rem(i, LOCAL)
            w = lax.rem(i, WEIGHTS)

            def sent(at, size):
                x = x_ref[pl.ds(send_at + at, size), :]
                for k, weight in enumerate((gate_w, up_w)):
                    near_send[s, pl.ds(at, size), k * chunk:(k + 1) * chunk] = jnp.dot(
                        x, weight[w], preferred_element_type=jnp.float32
                    ).astype(jnp.bfloat16)

            for_pieces(half, sent)
            near_copy(i).start()

            def kept(at, size):
                x = x_ref[pl.ds(keep_at + at, size), :]
                for k, weight in enumerate((gate_w, up_w)):
                    keep[s, pl.ds(at, size), k * chunk:(k + 1) * chunk] = jnp.dot(
                        x, weight[w], preferred_element_type=jnp.float32
                    )

            for_pieces(half, kept)

        @pl.when((i >= 1) & (i - 1 < steps))
        def _():
            j = i - 1
            s, r = lax.rem(j, LOCAL), lax.rem(j, RECV)
            near_copy(j).wait()

            def summed(at, size):
                far_send[s, pl.ds(at, size), :] = (
                    keep[s, pl.ds(other_in + at, size), :]
                    + near_recv[r, pl.ds(other_in + at, size), :].astype(jnp.float32)
                ).astype(jnp.bfloat16)

            for_pieces(quarter, summed)
            far_copy(j).start()

            def held(at, size):
                own[s, pl.ds(at, size), :] = (
                    keep[s, pl.ds(mine_in + at, size), :]
                    + near_recv[r, pl.ds(mine_in + at, size), :].astype(jnp.float32)
                )

            for_pieces(quarter, held)

        @pl.when((i >= 3) & (i - 3 < steps))
        def _():
            j = i - 3
            s, r = lax.rem(j, LOCAL), lax.rem(j, RECV)
            far_copy(j).wait()

            def activate(at, size):
                both = own[s, pl.ds(at, size), :] + far_recv[r, pl.ds(at, size), :].astype(jnp.float32)
                gate_pre = both[:, :chunk]
                up_pre = both[:, chunk:]
                hidden[r, pl.ds(mine + at, size), :] = (
                    gate_pre / (1.0 + jnp.exp(-gate_pre)) * up_pre
                ).astype(jnp.bfloat16)

            for_pieces(quarter, activate)
            share_copy(j).start()
            give_copy(j).start()

        @pl.when((i >= 5) & (i - 5 < steps))
        def _():
            share_copy(i - 5).wait()
            pass_copy(i - 5).start()

        @pl.when((i >= 6) & (i - 6 < steps))
        def _():
            j = i - 6
            r, w = lax.rem(j, RECV), lax.rem(j, WEIGHTS)
            give_copy(j).wait()
            pass_copy(j).wait()
            load_down(j).wait()

            def add(at, size):
                total[pl.ds(at, size), :] += jnp.dot(
                    hidden[r, pl.ds(at, size), :], down_w[w], preferred_element_type=jnp.float32
                )

            for_pieces(rows, add)

        return carry

    lax.fori_loop(0, steps + 6, iteration, 0)

    def finish(at, size):
        out_ref[pl.ds(at, size), :] = total[pl.ds(at, size), :].astype(jnp.bfloat16)

    for_pieces(rows, finish)


def expert_rows(received, gate_weight, up_weight, down_weight):
    rows, depth = received.shape
    width = gate_weight.shape[1]
    out = down_weight.shape[1]
    chunk = 256 if width % 256 == 0 else 128
    steps = width // chunk
    half, quarter = rows // 2, rows // 4
    vmem, hbm = pl.BlockSpec(memory_space=pltpu.VMEM), pl.BlockSpec(memory_space=pl.ANY)
    dma = pltpu.SemaphoreType.DMA
    bf16, f32 = jnp.bfloat16, jnp.float32
    return pl.pallas_call(
        functools.partial(expert_kernel, steps, chunk),
        out_shape=jax.ShapeDtypeStruct((rows, out), bf16),
        in_specs=[vmem, hbm, hbm, hbm],
        out_specs=vmem,
        scratch_shapes=[
            pltpu.VMEM((WEIGHTS, depth, chunk), bf16),
            pltpu.VMEM((WEIGHTS, depth, chunk), bf16),
            pltpu.VMEM((WEIGHTS, chunk, out), bf16),
            pltpu.VMEM((LOCAL, half, 2 * chunk), bf16),
            pltpu.VMEM((RECV, half, 2 * chunk), bf16),
            pltpu.VMEM((LOCAL, half, 2 * chunk), f32),
            pltpu.VMEM((LOCAL, quarter, 2 * chunk), bf16),
            pltpu.VMEM((RECV, quarter, 2 * chunk), bf16),
            pltpu.VMEM((LOCAL, quarter, 2 * chunk), f32),
            pltpu.VMEM((RECV, rows, chunk), bf16),
            pltpu.VMEM((rows, out), f32),
            dma((3, WEIGHTS)),
            dma((LOCAL,)), dma((RECV,)),
            dma((LOCAL,)), dma((RECV,)),
            dma((RECV,)), dma((RECV,)),
            dma((RECV,)), dma((RECV,)),
            dma((RECV,)), dma((RECV,)),
        ],
        compiler_params=pltpu.CompilerParams(
            collective_id=0, has_side_effects=True, vmem_limit_bytes=60 * 1024 * 1024
        ),
        cost_estimate=pl.CostEstimate(
            flops=2 * rows * width * (2 * depth + out),
            bytes_accessed=2 * width * (2 * depth + out),
            transcendentals=0,
        ),
    )(received, gate_weight, up_weight, down_weight)


def exchange_kernel(arrays, *refs):
    sends, recvs, sems = refs[:arrays], refs[arrays:2 * arrays], refs[2 * arrays:]
    send_sem, recv_sem, local_sem = sems
    count = sends[0].shape[0]
    me = lax.axis_index("ep")

    def peer_of(k):
        return lax.rem(me + k, count)

    barrier = pltpu.get_barrier_semaphore()

    def greet(k, carry):
        pl.semaphore_signal(barrier, inc=1, device_id={"ep": peer_of(k)}, device_id_type=MESH)
        return carry

    def copy(a, k):
        return pltpu.make_async_remote_copy(
            src_ref=sends[a].at[peer_of(k)], dst_ref=recvs[a].at[me],
            send_sem=send_sem.at[a, k], recv_sem=recv_sem.at[a, k],
            device_id={"ep": peer_of(k)}, device_id_type=MESH,
        )

    def begin(k, carry):
        for a in range(arrays):
            copy(a, k).start()
        return carry

    def end(k, carry):
        for a in range(arrays):
            copy(a, k).wait()
        return carry

    lax.fori_loop(1, count, greet, 0)
    stays = [
        pltpu.make_async_copy(sends[a].at[me], recvs[a].at[me], local_sem.at[a])
        for a in range(arrays)
    ]
    for stay in stays:
        stay.start()
    pl.semaphore_wait(barrier, count - 1)
    lax.fori_loop(1, count, begin, 0)
    lax.fori_loop(1, count, end, 0)
    for stay in stays:
        stay.wait()


def exchange(blocks, number):
    arrays, count = len(blocks), blocks[0].shape[0]
    dma = pltpu.SemaphoreType.DMA
    vmem = pl.BlockSpec(memory_space=pltpu.VMEM)
    return pl.pallas_call(
        functools.partial(exchange_kernel, arrays),
        out_shape=[jax.ShapeDtypeStruct(b.shape, b.dtype) for b in blocks],
        in_specs=[vmem] * arrays,
        out_specs=[vmem] * arrays,
        scratch_shapes=[dma((arrays, count)), dma((arrays, count)), dma((arrays,))],
        compiler_params=pltpu.CompilerParams(
            collective_id=number, has_side_effects=True, vmem_limit_bytes=60 * 1024 * 1024
        ),
    )(*blocks)


def per_device(tokens, expert_ids, gates, gate_weight, up_weight, down_weight):
    count_tok = tokens.shape[0]
    quarter = tokens.shape[1]
    replicas = lax.axis_size("ep") // EXPERTS
    slots_all = EXPERTS * CAP
    flat_ids = expert_ids.reshape(-1)
    onehot = (flat_ids[:, None] == jnp.arange(EXPERTS, dtype=jnp.int32)[None, :]).astype(jnp.int32)
    before = jnp.cumsum(onehot, axis=0) - onehot
    target = flat_ids * CAP + jnp.sum(before * onehot, axis=1)
    matches = (
        target.reshape(count_tok, TOP)[:, :, None]
        == jnp.arange(slots_all, dtype=jnp.int32)[None, None, :]
    ).astype(jnp.float32)
    combine = jnp.sum(matches * gates[:, :, None], axis=1)
    selector = jnp.sum(matches, axis=1).astype(jnp.bfloat16)
    dispatched = jnp.einsum(
        "ts,td->sd", selector, tokens, preferred_element_type=jnp.float32
    ).astype(jnp.bfloat16)
    copies = jnp.broadcast_to(
        dispatched.reshape(EXPERTS, 1, CAP, quarter), (EXPERTS, replicas, CAP, quarter)
    )
    counts = jnp.sum(onehot, axis=0).astype(jnp.float32)
    totals = jnp.sum(onehot.astype(jnp.float32) * gates.reshape(-1)[:, None], axis=0)
    stats = jnp.pad(jnp.stack((counts, totals)), ((0, 6), (0, 128 - EXPERTS)))
    stats = jnp.broadcast_to(stats[None], (lax.axis_size("ep"),) + stats.shape)
    received, stats = exchange((copies.reshape(-1, CAP, quarter), stats), 1)
    received = received.reshape(-1, quarter)
    partial_value = expert_rows(received, gate_weight, up_weight, down_weight)
    (returned,) = exchange((partial_value.reshape(-1, CAP, quarter),), 2)
    results = jnp.sum(returned.reshape(EXPERTS, replicas, CAP, quarter).astype(jnp.float32), axis=1)
    results = results.reshape(slots_all, quarter)
    mixed = jnp.dot(
        combine, results, precision=lax.Precision.HIGHEST, preferred_element_type=jnp.float32
    ).astype(jnp.bfloat16)
    stats = jnp.sum(stats, axis=0)
    counts, totals = stats[0, :EXPERTS], stats[1, :EXPERTS]
    tokens_all = count_tok * lax.axis_size("ep")
    aux_loss = EXPERTS * jnp.sum(counts / (TOP * tokens_all) * (totals / tokens_all))
    return (mixed, counts, aux_loss)


def solution(mesh):
    placed = (
        P("ep", "tp"),
        P("ep", None),
        P("ep", None),
        P("tp", "ep"),
        P("tp", "ep"),
        P("ep", "tp"),
    )
    return jax.shard_map(
        per_device, mesh=mesh, in_specs=placed, out_specs=(P("ep", "tp"), P(), P()), check_vma=False
    )
```
